32 devices in a mesh: sec: 4 (over y, x), bond: 8 (over z, core).
Axes of the slice: x: 2, y: 2, z: 4, core: 2. Of those that a mesh axis runs over, the one named last changes fastest.
Arguments:
- left_vectors: bfloat16 [128, 4096], P(None, 'bond'), may hold values from -6 to 6
- site_tensors: bfloat16 [4, 4096, 4, 4096], P('sec', None, None, 'bond'), may hold values from -0.09375 to 0.09375
- displacement: float32 [128, 216], P('sec'), may hold values from -2.5 to 2.5
- photon_counts: int32 [128, 216], P('sec'), may hold values from 0 to 3
- mode_order: int32 [216], replicated, may hold values from 0 to 215, each once
Outputs:
- log_likelihood: float32 [4, 128], P('sec')
- log_norm: float32 [4, 128], P('sec')
The draws below stay inside these ranges and needn't reach their ends.
Inputs may be any that keep to these rules, and one draw needn't show every extreme that they name: `mode_order`: each of the 216 modes appears once.
All inputs are finite; a program needn't handle non-finite values.
Results may differ from the reference program's by a relative error of at most 0.0015.
Values may be sent and summed in bfloat16 or wider, within the bound.
No kernel may reach another device: no remote copies, remote signals or barrier semaphores. Data moves between devices by JAX's collectives and lax.ppermute only.
A program may use at most 64 MiB of HBM per device.

```python
import math
import jax
import jax.numpy as jnp
from jax import lax

CHI = 4096
CUT = 4
MODE_POOL = 216
SAMPLES = 128
MODES = 4


def with_ends(result, own_key, smallest, top_value):
    index_at = [jax.random.randint(jax.random.fold_in(own_key, axis), (), 0, length) for axis, length in enumerate(result.shape)]
    longest = result.shape.index(max(result.shape))
    neighbour = index_at[:longest] + [(index_at[longest] + 1) % result.shape[longest]] + index_at[longest + 1:]
    return result.at[tuple(index_at)].set(smallest).at[tuple(neighbour)].set(top_value)


def block_scale(stream_key, shape, split, low, largest):
    def one(position, shards_of):
        draws = jax.random.uniform(jax.random.fold_in(jax.random.fold_in(stream_key, 6), position), (shards_of,), jnp.float32, low / len(split), largest / len(split))
        return jnp.repeat(jnp.exp(draws), shape[position] // shards_of).reshape((-1,) + (1,) * (len(shape) - position - 1))

    level = one(*split[0])
    for cut in split[1:]:
        level = level * one(*cut)
    return level


def centred(stream_key, shape, width, reach, split=(), held_as=jnp.bfloat16):
    drawn = jax.random.normal(stream_key, shape, jnp.float32) * width
    if len(split) > 0:
        drawn = block_scale(stream_key, shape, split, -0.22, 0.18) * drawn
    return jnp.clip(drawn, min=-reach, max=reach).astype(held_as)


def setup_inputs(seed: int = 0) -> dict:
    splits = jax.random.split(jax.random.key(seed), 6)
    left_vectors = centred(splits[0], (SAMPLES, CHI), 1.0, 6.0, ((1, 8),))
    site_tensors = centred(splits[1], (MODES, CHI, CUT, CHI), CHI ** -0.5, 0.09375, ((0, 4), (3, 8)))
    displacement = centred(splits[2], (SAMPLES, MODE_POOL), 0.7, 2.5, ((0, 4),), jnp.float32)
    photon_counts = with_ends(jax.random.randint(splits[3], (SAMPLES, MODE_POOL), 0, CUT), jax.random.fold_in(splits[3], 1), 0, CUT - 1).astype(jnp.int32)
    mode_order = jax.random.permutation(splits[4], MODE_POOL).astype(jnp.int32)
    return {"left_vectors": left_vectors, "site_tensors": site_tensors, "displacement": displacement, "photon_counts": photon_counts, "mode_order": mode_order}


epsilon = 1e-06

def displacement_table(cutoff):
    table = [[[0.0 for degree_slot in range(2 * cutoff - 1)] for col_level in range(cutoff)] for row_level in range(cutoff)]
    for row_level in range(cutoff):
        for col_level in range(cutoff):
            lower = min(row_level, col_level)
            upper = max(row_level, col_level)
            excess = upper - lower
            parity = 1.0 if row_level >= col_level else (-1.0) ** excess
            prefactor = math.sqrt(math.factorial(lower) / math.factorial(upper))
            for term in range(lower + 1):
                table[row_level][col_level][excess + 2 * term] += parity * prefactor * (-1.0) ** term * math.comb(upper, lower - term) / math.factorial(term)
    return table

def displacement_matrix(amplitude):
    table = jnp.asarray(displacement_table(CUT), dtype=jnp.float32)
    power_list = [jnp.ones_like(amplitude)]
    for degree in range(2 * CUT - 2):
        power_list.append(power_list[-1] * amplitude)
    power_stack = jnp.stack(power_list, axis=1)
    poly = jnp.einsum('sp,mnp->smn', power_stack, table, precision=lax.Precision.HIGHEST)
    return jnp.exp(-0.5 * amplitude * amplitude)[:, None, None] * poly

def reference(left_vectors, site_tensors, displacement, photon_counts, mode_order):
    vectors = left_vectors
    factor = jnp.ones((left_vectors.shape[0],), jnp.float32)
    levels = jnp.arange(CUT).astype(jnp.float32)
    results = []
    norms = []
    for segment_index in range(MODES):
        column = mode_order[segment_index]
        amplitude = jnp.take(displacement, column, axis=1)
        counted = jnp.take(photon_counts, column, axis=1).astype(jnp.float32)
        matrix = site_tensors[segment_index].reshape(CHI, CUT * CHI)
        projected = jnp.dot(vectors, matrix, preferred_element_type=jnp.float32) * factor[:, None]
        projected = projected.reshape(-1, CUT, CHI)
        shifts = displacement_matrix(amplitude)
        displaced = jnp.einsum('smn,snb->smb', shifts, projected, precision=lax.Precision.HIGHEST)
        weights = lax.optimization_barrier(jnp.sum(displaced * displaced, axis=2))
        select = (counted[:, None] == levels[None, :]).astype(jnp.float32)
        chosen_weight = lax.optimization_barrier(jnp.sum(select * weights, axis=1))
        results.append(jnp.log(chosen_weight) - jnp.log(lax.optimization_barrier(jnp.sum(weights, axis=1))))
        norms.append(jnp.log(chosen_weight / CHI + epsilon))
        factor = lax.rsqrt(chosen_weight / CHI + epsilon)
        chosen = lax.optimization_barrier(jnp.sum(select[:, :, None] * displaced, axis=1))
        vectors = chosen.astype(jnp.bfloat16)
    return (jnp.stack(results), jnp.stack(norms))
```

```python
import functools
import math

import jax
import jax.numpy as jnp
from jax import lax
from jax.experimental import pallas as pl
from jax.experimental.pallas import tpu as pltpu
from jax.sharding import PartitionSpec as P

epsilon = 1e-06
EXTRA = 8


def swapped(x, axis, mask):
    size = lax.axis_size(axis)
    return lax.ppermute(x, axis, [(i, i ^ mask) for i in range(size)])


def displacement_table(cutoff):
    table = [
        [[0.0 for degree_slot in range(2 * cutoff - 1)] for col_level in range(cutoff)]
        for row_level in range(cutoff)
    ]
    for row_level in range(cutoff):
        for col_level in range(cutoff):
            lower = min(row_level, col_level)
            upper = max(row_level, col_level)
            excess = upper - lower
            parity = 1.0 if row_level >= col_level else (-1.0) ** excess
            prefactor = math.sqrt(math.factorial(lower) / math.factorial(upper))
            for term in range(lower + 1):
                table[row_level][col_level][excess + 2 * term] += (
                    parity
                    * prefactor
                    * (-1.0) ** term
                    * math.comb(upper, lower - term)
                    / math.factorial(term)
                )
    return table


def displacement_matrix(amplitude, cutoff):
    table = jnp.asarray(displacement_table(cutoff), dtype=jnp.float32)
    power_list = [jnp.ones_like(amplitude)]
    for degree in range(2 * cutoff - 2):
        power_list.append(power_list[-1] * amplitude)
    power_stack = jnp.stack(power_list, axis=1)
    poly = jnp.einsum("sp,mnp->smn", power_stack, table, precision=lax.Precision.HIGHEST)
    return jnp.exp(-0.5 * amplitude * amplitude)[:, None, None] * poly


def split_kernel(chunk, slots, source, out, held, sems):
    full, cutoff, width = source.shape[1:]
    count = full // chunk

    def copy(index, slot):
        rows = pl.ds(pl.multiple_of(index * chunk, chunk), chunk)
        return pltpu.make_async_copy(source.at[0, rows], held.at[slot], sems.at[slot])

    for index in range(min(slots - 1, count)):
        copy(index, index).start()

    def step(index, carry):
        slot = lax.rem(index, slots)

        @pl.when(index + slots - 1 < count)
        def _():
            ahead = index + slots - 1
            copy(ahead, lax.rem(ahead, slots)).start()

        copy(index, slot).wait()
        rows = pl.ds(pl.multiple_of(index * chunk, chunk), chunk)
        out[rows, :] = pltpu.einshape("inb->i(nb)", held[slot])
        return carry

    lax.fori_loop(0, count, step, 0)


def split_levels(site):
    full, cutoff, width = site.shape[1:]
    chunk = 256
    slots = 3
    return pl.pallas_call(
        functools.partial(split_kernel, chunk, slots),
        in_specs=[pl.BlockSpec(memory_space=pltpu.HBM)],
        out_specs=pl.BlockSpec(memory_space=pltpu.VMEM),
        out_shape=pltpu.VMEM((full, cutoff * width), site.dtype),
        scratch_shapes=[
            pltpu.VMEM((slots, chunk, cutoff, width), site.dtype),
            pltpu.SemaphoreType.DMA((slots,)),
        ],
        compiler_params=pltpu.CompilerParams(vmem_limit_bytes=24 << 20),
        cost_estimate=pl.CostEstimate(
            flops=16_000_000_000, bytes_accessed=site.size * 2, transcendentals=0
        ),
        name="split_levels",
    )(site)


def section_kernel(turn, cutoff, where_ref, *refs):
    pieces = refs[: len(refs) - 7]
    matrix, coef, kept, next_ref, weights_ref, joined, projected = refs[len(pieces) :]
    samples, width = pieces[0].shape
    if turn:
        samples -= EXTRA
    full = matrix.shape[0]
    bond = where_ref[1]
    for mask, piece in enumerate(pieces):
        place = bond ^ mask if len(pieces) <= 8 else lax.rem(bond + mask, len(pieces))
        start = pl.multiple_of(place * width, width)
        joined[:, pl.ds(start, width)] = piece[:samples, :]

    block = 256

    def columns(index, carry):
        at = pl.ds(pl.multiple_of(index * block, block), block)
        projected[:, at] = jnp.dot(joined[...], matrix[:, at], preferred_element_type=jnp.float32)
        return carry

    lax.fori_loop(0, cutoff * width // block, columns, 0)

    if turn:
        total = jnp.zeros((1, samples), jnp.float32)
        for piece in pieces:
            rows = piece[samples:, :samples].astype(jnp.float32)
            total += rows[0:1] + rows[1:2] + rows[2:3]
        factor_row = lax.rsqrt(total / full + epsilon)
        factor = jnp.transpose(jnp.broadcast_to(factor_row, (samples, samples)))[:, :1]
    g = jnp.transpose(coef[...])
    if turn:
        g = g * factor
    lane = lax.broadcasted_iota(jnp.int32, (samples, 128), 1)
    parts = [projected[:, n * width : (n + 1) * width] for n in range(cutoff)]
    sums = jnp.zeros((samples, 128), jnp.float32)
    for m in range(cutoff + 1):
        value = g[:, m * cutoff : m * cutoff + 1] * parts[0]
        for n in range(1, cutoff):
            value += g[:, m * cutoff + n : m * cutoff + n + 1] * parts[n]
        total = jnp.sum(value * value, axis=1, keepdims=True)
        sums = jnp.where(lane == m, total, sums)
        if m == cutoff:
            next_ref[:samples, :] = value.astype(next_ref.dtype)
    rows = jnp.transpose(sums)[:8, :samples]
    weights_ref[...] = jnp.where(where_ref[0] == turn, rows, kept[...])
    norm = rows[cutoff : cutoff + 1]
    high = norm.astype(jnp.bfloat16).astype(jnp.float32)
    middle = (norm - high).astype(jnp.bfloat16).astype(jnp.float32)
    low = norm - high - middle
    pick = lax.broadcasted_iota(jnp.int32, (EXTRA, samples), 0)
    tail = jnp.where(pick == 0, high, jnp.where(pick == 1, middle, jnp.where(pick == 2, low, 0.0)))
    next_ref[samples:, :samples] = tail.astype(next_ref.dtype)
    if width > samples:
        next_ref[samples:, samples:] = jnp.zeros((EXTRA, width - samples), next_ref.dtype)


def section(turn, cutoff, where, pieces, matrix, coef, kept):
    samples = coef.shape[1]
    width = pieces[0].shape[1]
    full = matrix.shape[0]
    vmem = pl.BlockSpec(memory_space=pltpu.VMEM)
    return pl.pallas_call(
        functools.partial(section_kernel, turn, cutoff),
        in_specs=[pl.BlockSpec(memory_space=pltpu.SMEM)] + [vmem] * (len(pieces) + 3),
        out_specs=[vmem, vmem],
        out_shape=[
            jax.ShapeDtypeStruct((samples + EXTRA, width), jnp.bfloat16),
            jax.ShapeDtypeStruct((8, samples), jnp.float32),
        ],
        scratch_shapes=[
            pltpu.VMEM((samples, full), jnp.bfloat16),
            pltpu.VMEM((samples, cutoff * width), jnp.float32),
        ],
        compiler_params=pltpu.CompilerParams(vmem_limit_bytes=26 << 20),
        cost_estimate=pl.CostEstimate(
            flops=2 * samples * full * cutoff * width, bytes_accessed=4 << 20, transcendentals=0
        ),
        name=f"section_{turn}",
    )(where, *pieces, matrix, coef, kept)


def gathered(piece, axis):
    size = lax.axis_size(axis)
    if size > 8 or size & (size - 1):
        every = lax.all_gather(piece, axis)
        index = lax.axis_index(axis)
        return [
            lax.dynamic_index_in_dim(every, (index + step) % size, 0, keepdims=False)
            for step in range(size)
        ]
    even = [piece] + [swapped(piece, axis, mask) for mask in range(2, size, 2)]
    odd = [swapped(part, axis, 1) for part in even]
    pieces = []
    for first, second in zip(even, odd):
        pieces += [first, second]
    return pieces


def local(left_vectors, site_tensors, displacement, photon_counts, mode_order):
    full_width = site_tensors.shape[1]
    cutoff = site_tensors.shape[2]
    samples = left_vectors.shape[0]
    segment_count = lax.axis_size("sec")
    segment_index = lax.axis_index("sec")
    bond_index = lax.axis_index("bond")
    where = jnp.stack([segment_index, bond_index]).astype(jnp.int32)

    pieces = gathered(left_vectors, "bond")

    stacked = jnp.stack([displacement, photon_counts.astype(jnp.float32)])
    mode_total = displacement.shape[1]
    window_order = mode_order[:segment_count]
    picker = (window_order[None, :] == jnp.arange(mode_total, dtype=jnp.int32)[:, None]).astype(
        jnp.float32
    )
    ordered = jnp.einsum("rsm,mj->rsj", stacked, picker, precision=lax.Precision.HIGHEST)
    columns = lax.all_to_all(ordered, "sec", split_axis=2, concat_axis=1, tiled=True)
    shifts = displacement_matrix(columns[0, :, 0], cutoff)
    counts = columns[1, :, 0]
    levels = jnp.arange(cutoff).astype(jnp.float32)
    select = (counts[:, None] == levels[None, :]).astype(jnp.float32)
    chosen_shift = jnp.sum(select[:, :, None] * shifts, axis=1)
    coef = jnp.concatenate([shifts.reshape(samples, cutoff * cutoff), chosen_shift], axis=1)
    coef = jnp.transpose(jnp.pad(coef, ((0, 0), (0, -coef.shape[1] % 8))))

    coef, site_tensors = lax.optimization_barrier((coef, site_tensors))
    matrix = split_levels(site_tensors)
    kept = jnp.zeros((8, samples), jnp.float32)
    for turn in range(segment_count):
        vector, kept = section(turn, cutoff, where, pieces, matrix, coef, kept)
        if turn + 1 < segment_count:
            vector = swapped(vector, "sec", turn ^ (turn + 1))
            pieces = gathered(vector, "bond")

    weights = sum(gathered(kept, "bond"))[:cutoff]
    chosen_weight = jnp.sum(jnp.transpose(select) * weights, axis=0)
    log_prob = jnp.log(chosen_weight) - jnp.log(jnp.sum(weights, axis=0))
    log_scale = jnp.log(chosen_weight / full_width + epsilon)
    return (log_prob[None, :], log_scale[None, :])


def solution(mesh):
    placed = (P(None, "bond"), P("sec", None, None, "bond"), P("sec", None), P("sec", None), P())
    return jax.shard_map(
        local,
        mesh=mesh,
        in_specs=placed,
        out_specs=(P("sec", None), P("sec", None)),
        check_vma=False,
    )
```
